128 devices in a mesh: mode: 32 (over y_lo, z, x), var: 4 (over y_hi, core).
Axes of the slice: x: 4, y: 4 (y_hi: 2, y_lo: 2; y = y_hi * 2 + y_lo), z: 4, core: 2. Of those that a mesh axis runs over, the one named last changes fastest.
Arguments:
- control: bfloat16 [1, 4, 32, 1024, 1024], P(None, 'var', 'mode'), may hold values from -6 to 6
- filters: bfloat16 [3, 1024, 1024], replicated, may hold values from -4 to 5
- weights: bfloat16 [4, 3, 1024, 1024], P('var'), may hold values from 0.29882812 to 3
- vertical: bfloat16 [4, 64, 32], replicated, may hold values from -1 to 1
- balance: bfloat16 [3, 64, 64], replicated, may hold values from -0.75 to 0.75
Outputs:
- increment: bfloat16 [1, 4, 64, 1024, 1024], P(None, 'var', 'mode')
The draws below stay inside these ranges and needn't reach their ends.
All inputs are finite; a program needn't handle non-finite values.
Results may differ from the reference program's by a relative error of at most 0.006.
Values may be sent and summed in bfloat16 or wider, within the bound.
No kernel may reach another device: no remote copies, remote signals or barrier semaphores. Data moves between devices by JAX's collectives and lax.ppermute only.
A program may use at most 64 MiB of HBM per device.

```python
import math
import jax
import jax.numpy as jnp
from jax import lax

MEMBERS = 1
NX = 1024
LEV = 64
FILTERS = 3
MODES = 32
VARS = 4


def draw_filters(key, part):
    index = jnp.arange(NX, dtype=jnp.float32)
    gap = index[:, None] - index[None, :]
    dense_scale = 0.25 / jnp.sqrt(jnp.float32(NX))
    mats = []
    for k, ratio in enumerate([128, 32, 8]):
        spread = NX / ratio
        envelope = jnp.exp(-(gap * gap) / (2.0 * spread * spread))
        scale_term = 1.0 / jnp.sqrt(spread * 1.7724539)
        sub = jax.random.fold_in(key, 11 + k)
        far_key = jax.random.fold_in(key, 31 + k)
        noise = jnp.clip(jax.random.normal(sub, (NX, NX), jnp.float32), -4.0, 4.0)
        dense = jnp.clip(jax.random.normal(far_key, (NX, NX), jnp.float32), -4.0, 4.0)
        mats.append(jnp.eye(NX, dtype=jnp.float32) + scale_term * envelope * noise + dense_scale * dense)
    return jnp.stack(mats).astype(jnp.bfloat16)


def block_levels(stream_key, shape, split, least, high):
    loudness = 1.0
    for axis_at, blocks in split:
        draws = jax.random.uniform(jax.random.fold_in(jax.random.fold_in(stream_key, 6), axis_at), (blocks,), jnp.float32, least / len(split), high / len(split))
        loudness = loudness * jnp.repeat(jnp.exp(draws), shape[axis_at] // blocks).reshape((-1,) + (1,) * (len(shape) - 1 - axis_at))
    return loudness


def centred(key, shape, scale, limit, split=(), kind=jnp.bfloat16):
    level = block_levels(key, shape, split, -0.22, 0.18) if split else 1.0
    drawn = jax.random.normal(key, shape, jnp.float32) * scale * level
    return jnp.minimum(jnp.maximum(drawn, -limit), limit).astype(kind)


def setup_inputs(seed: int = 0) -> dict:
    streams_of = jax.random.split(jax.random.key(seed), 6)
    return {
        "control": centred(streams_of[0], (MEMBERS, VARS, MODES, NX, NX), 1.0, 6.0, ((1, 4), (2, 32))),
        "filters": draw_filters(jax.random.fold_in(streams_of[5], 71), 0),
        "weights": jnp.clip(jnp.exp(math.log(3.0) - 2.306499 * jax.random.uniform(streams_of[2], (VARS, FILTERS, NX, NX), jnp.float32) ** block_levels(streams_of[2], (VARS, FILTERS, NX, NX), ((0, 4),), -0.2, 0.2)), 0.29882812, 3.0).astype(jnp.bfloat16),
        "vertical": centred(streams_of[3], (VARS, LEV, MODES), MODES ** -0.5, 1.0),
        "balance": centred(streams_of[4], (VARS - 1, LEV, LEV), LEV ** -0.5, 0.75),
    }


def smooth_plane(plane, filters, weights):
    total = jnp.zeros(plane.shape, jnp.float32)
    for k in range(FILTERS):
        half = jnp.dot(filters[k], plane, preferred_element_type=jnp.float32).astype(jnp.bfloat16)
        full = jnp.dot(half, filters[k].T, preferred_element_type=jnp.float32)
        total = total + weights[k].astype(jnp.float32) * full
    return total.astype(jnp.bfloat16)


def reference(control, filters, weights, vertical, balance):
    results = []
    for m in range(MEMBERS):
        filtered = []
        for v in range(VARS):
            planes = lax.map(lambda p: smooth_plane(p, filters, weights[v]), control[m, v])
            filtered.append(planes.reshape(MODES, NX * NX))
        stream_levels = jnp.dot(vertical[0], filtered[0], preferred_element_type=jnp.float32)
        stream = stream_levels.astype(jnp.bfloat16)
        outs = [stream]
        for v in range(1, VARS):
            levels = jnp.dot(vertical[v], filtered[v], preferred_element_type=jnp.float32)
            extra = jnp.dot(balance[v - 1], stream, preferred_element_type=jnp.float32)
            outs.append((levels + extra).astype(jnp.bfloat16))
        results.append(jnp.stack(outs).reshape(VARS, LEV, NX, NX))
    return jnp.stack(results)
```

```python
import jax
import jax.numpy as jnp
from jax import lax
from jax.experimental import pallas as pl
from jax.experimental.pallas import tpu as pltpu
from jax.sharding import PartitionSpec as P

SUB = 8
WIDE = 256
MB = 2**20


def vmem(mib):
    return pltpu.CompilerParams(vmem_limit_bytes=mib * MB)


def cost(flops, nbytes):
    return pl.CostEstimate(flops=int(flops), bytes_accessed=int(nbytes), transcendentals=0)


def spread(small, contract):
    cols = small.shape[contract]
    rows = small.shape[1 - contract]
    wide = cols * SUB
    lane = lax.broadcasted_iota(jnp.int32, (cols, wide), 1)
    source = lax.broadcasted_iota(jnp.int32, (cols, wide), 0)
    repeat = jnp.where(lane // SUB == source, 1.0, 0.0).astype(jnp.bfloat16)
    each = lax.dot_general(
        small, repeat, (((contract,), (0,)), ((), ())), preferred_element_type=jnp.float32
    )
    sub = lax.broadcasted_iota(jnp.int32, (rows, SUB, wide), 1)
    at = lax.broadcasted_iota(jnp.int32, (rows, SUB, wide), 2)
    tall = jnp.broadcast_to(each[:, None, :], (rows, SUB, wide))
    return jnp.where(at % SUB == sub, tall, 0.0).reshape(rows * SUB, wide).astype(jnp.bfloat16)


def smooth_kernel(
    plane_any, filters_any, weights_any, vertical_any, balance_any,
    out_ref, coeff_ref,
    plane_ref, filters_ref, weights_ref, vertical_ref, balance_ref, half_ref, total_ref, sems,
):
    count = filters_ref.shape[0]
    small = [
        pltpu.make_async_copy(vertical_any, vertical_ref, sems.at[2 * count + 1]),
        pltpu.make_async_copy(balance_any, balance_ref, sems.at[2 * count + 2]),
    ]
    plane = pltpu.make_async_copy(plane_any, plane_ref, sems.at[2 * count])
    filters = [
        pltpu.make_async_copy(filters_any.at[k], filters_ref.at[k], sems.at[2 * k])
        for k in range(count)
    ]
    weights = [
        pltpu.make_async_copy(weights_any.at[k], weights_ref.at[k], sems.at[2 * k + 1])
        for k in range(count)
    ]
    for copy in small:
        copy.start()
    plane.start()
    for k in range(count):
        filters[k].start()
        weights[k].start()

    for copy in small:
        copy.wait()
    modes = vertical_ref.shape[1] * SUB
    for v in range(vertical_ref.shape[0]):
        coeff_ref[v, :, :modes] = spread(vertical_ref[v], 0)
        if v:
            coeff_ref[v, :, modes:] = spread(balance_ref[v - 1], 1)

    plane.wait()
    for k in range(count):
        filters[k].wait()
        half_ref[...] = jnp.dot(
            filters_ref[k], plane_ref[...], preferred_element_type=jnp.float32
        ).astype(jnp.bfloat16)
        weights[k].wait()
        full = lax.dot_general(
            half_ref[...], filters_ref[k], (((1,), (1,)), ((), ())),
            preferred_element_type=jnp.float32,
        )
        term = weights_ref[k].astype(jnp.float32) * full
        if k == 0:
            total_ref[...] = term
        elif k < count - 1:
            total_ref[...] += term
        else:
            out_ref[...] = (total_ref[...] + term).astype(jnp.bfloat16)


def smooth(plane, filters, weights, vertical, balance):
    count, size, _ = filters.shape
    nvar, modes, levs = vertical.shape
    return pl.pallas_call(
        smooth_kernel,
        out_shape=[
            jax.ShapeDtypeStruct((size, size), jnp.bfloat16),
            jax.ShapeDtypeStruct((nvar, levs * SUB, (modes + levs) * SUB), jnp.bfloat16),
        ],
        in_specs=[pl.BlockSpec(memory_space=pl.ANY)] * 5,
        scratch_shapes=[
            pltpu.VMEM(plane.shape, jnp.bfloat16),
            pltpu.VMEM(filters.shape, jnp.bfloat16),
            pltpu.VMEM(weights.shape, jnp.bfloat16),
            pltpu.VMEM(vertical.shape, jnp.bfloat16),
            pltpu.VMEM(balance.shape, jnp.bfloat16),
            pltpu.VMEM((size, size), jnp.bfloat16),
            pltpu.VMEM((size, size), jnp.float32),
            pltpu.SemaphoreType.DMA((2 * count + 3,)),
        ],
        cost_estimate=cost(4 * count * size**3, 18 * MB),
        compiler_params=pltpu.CompilerParams(vmem_limit_bytes=67043328),
        name="smooth",
    )(plane, filters, weights, vertical, balance)


def level_kernel(blocks_ref, coeff_ref, out_ref):
    nvar, modes, _, size = blocks_ref.shape
    deep = modes * SUB
    for first in range(0, size, WIDE):
        lanes = slice(first, first + WIDE)
        stream = None
        for v in range(nvar):
            block = blocks_ref[v, :, :, lanes].reshape(deep, WIDE)
            if v == 0:
                level = jnp.dot(coeff_ref[v, :, :deep], block, preferred_element_type=jnp.float32)
                level = stream = level.astype(jnp.bfloat16)
            else:
                level = jnp.dot(
                    coeff_ref[v],
                    jnp.concatenate([block, stream], axis=0),
                    preferred_element_type=jnp.float32,
                ).astype(jnp.bfloat16)
            shape = (out_ref.shape[1], out_ref.shape[2], SUB, WIDE)
            out_ref[v, :, :, :, lanes] = level.reshape(shape)


def mix_levels(blocks, coeff, nmode):
    nvar, modes, _, size = blocks.shape
    tall = coeff.shape[1]
    each = tall // SUB // nmode
    return pl.pallas_call(
        level_kernel,
        out_shape=jax.ShapeDtypeStruct((nvar, nmode, each, SUB, size), jnp.bfloat16),
        cost_estimate=cost(
            2 * tall * size * (nvar * modes * SUB + (nvar - 1) * tall), 8 * MB
        ),
        compiler_params=vmem(32),
        name="levels",
    )(blocks, coeff)


def place_kernel(back_ref, out_any, sems):
    tiles, levs = back_ref.shape[:2]
    some = tiles // sems.shape[1]
    copies = []
    for at in range(levs):
        for i in range(sems.shape[1]):
            rows = pl.ds(i * some, some)
            copies.append(
                pltpu.make_async_copy(back_ref.at[rows, at], out_any.at[at, rows], sems.at[at, i])
            )
    for copy in copies:
        copy.start()
    for copy in copies:
        copy.wait()


def place(back):
    tiles, levs, sub, size = back.shape
    return pl.pallas_call(
        place_kernel,
        out_shape=jax.ShapeDtypeStruct((levs, tiles, sub, size), jnp.bfloat16),
        in_specs=[pl.BlockSpec(memory_space=pltpu.VMEM)],
        out_specs=pl.BlockSpec(memory_space=pl.ANY),
        scratch_shapes=[pltpu.SemaphoreType.DMA((levs, 8))],
        cost_estimate=cost(2**29, 8 * MB),
        compiler_params=vmem(16),
        name="place",
    )(back)


def per_device(control, filters, weights, vertical, balance):
    size = control.shape[-1]
    nmode, nvar = lax.axis_size("mode"), lax.axis_size("var")
    count = nmode * nvar
    each = vertical.shape[1] // nmode
    axes = ("var", "mode")
    filtered, coeff = smooth(
        control[0, 0, 0], filters, weights[0], jnp.swapaxes(vertical, 1, 2), balance
    )
    blocks = lax.all_to_all(filtered.reshape(count, SUB, size), axes, 0, 0, tiled=True)
    result = mix_levels(blocks.reshape(nvar, nmode, SUB, size), coeff, nmode)
    back = lax.all_to_all(result.reshape(count, each, SUB, size), axes, 0, 0, tiled=True)
    return place(back).reshape(1, 1, each, size, size)


def solution(mesh):
    in_specs = (P(None, "var", "mode", None, None), P(), P("var", None, None, None), P(), P())
    out_specs = P(None, "var", "mode", None, None)
    return jax.shard_map(
        per_device, mesh=mesh, in_specs=in_specs, out_specs=out_specs, check_vma=False
    )
```

```python
import jax
import jax.numpy as jnp
from jax import lax
from jax.experimental import pallas as pl
from jax.experimental.pallas import tpu as pltpu
from jax.sharding import PartitionSpec as P

SUB = 8
WIDE = 256
MB = 2**20


def vmem(mib):
    return pltpu.CompilerParams(vmem_limit_bytes=mib * MB)


def cost(flops, nbytes):
    return pl.CostEstimate(flops=int(flops), bytes_accessed=int(nbytes), transcendentals=0)


def spread(small, contract):
    cols = small.shape[contract]
    rows = small.shape[1 - contract]
    wide = cols * SUB
    lane = lax.broadcasted_iota(jnp.int32, (cols, wide), 1)
    source = lax.broadcasted_iota(jnp.int32, (cols, wide), 0)
    repeat = jnp.where(lane // SUB == source, 1.0, 0.0).astype(jnp.bfloat16)
    each = lax.dot_general(
        small, repeat, (((contract,), (0,)), ((), ())), preferred_element_type=jnp.float32
    )
    sub = lax.broadcasted_iota(jnp.int32, (rows, SUB, wide), 1)
    at = lax.broadcasted_iota(jnp.int32, (rows, SUB, wide), 2)
    tall = jnp.broadcast_to(each[:, None, :], (rows, SUB, wide))
    return jnp.where(at % SUB == sub, tall, 0.0).reshape(rows * SUB, wide).astype(jnp.bfloat16)


def smooth_kernel(
    plane_any, filters_any, weights_any,
    out_ref,
    plane_ref, filters_ref, weights_ref, half_ref, total_ref,
    sems,
):
    count = filters_ref.shape[0]
    plane = pltpu.make_async_copy(plane_any, plane_ref, sems.at[2 * count])
    filters = [
        pltpu.make_async_copy(filters_any.at[k], filters_ref.at[k], sems.at[2 * k])
        for k in range(count)
    ]
    weights = [
        pltpu.make_async_copy(weights_any.at[k], weights_ref.at[k], sems.at[2 * k + 1])
        for k in range(count)
    ]
    plane.start()
    for k in range(count):
        filters[k].start()
        weights[k].start()

    plane.wait()
    for k in range(count):
        filters[k].wait()
        half_ref[...] = jnp.dot(
            filters_ref[k], plane_ref[...], preferred_element_type=jnp.float32
        ).astype(jnp.bfloat16)
        weights[k].wait()
        full = lax.dot_general(
            half_ref[...], filters_ref[k], (((1,), (1,)), ((), ())),
            preferred_element_type=jnp.float32,
        )
        term = weights_ref[k].astype(jnp.float32) * full
        if k == 0:
            total_ref[...] = term
        elif k < count - 1:
            total_ref[...] += term
        else:
            out_ref[...] = (total_ref[...] + term).astype(jnp.bfloat16)


def smooth(plane, filters, weights):
    count, size, _ = filters.shape
    return pl.pallas_call(
        smooth_kernel,
        out_shape=jax.ShapeDtypeStruct((size, size), jnp.bfloat16),
        in_specs=[pl.BlockSpec(memory_space=pl.ANY)] * 3,
        scratch_shapes=[
            pltpu.VMEM(plane.shape, jnp.bfloat16),
            pltpu.VMEM(filters.shape, jnp.bfloat16),
            pltpu.VMEM(weights.shape, jnp.bfloat16),
            pltpu.VMEM((size, size), jnp.bfloat16),
            pltpu.VMEM((size, size), jnp.float32),
            pltpu.SemaphoreType.DMA((2 * count + 1,)),
        ],
        cost_estimate=cost(4 * count * size**3, 18 * MB),
        compiler_params=pltpu.CompilerParams(vmem_limit_bytes=52428800),
        name="smooth",
    )(plane, filters, weights)


def level_kernel(blocks_ref, vertical_ref, balance_ref, out_ref, coeff_ref):
    nvar, modes, _, size = blocks_ref.shape
    deep = modes * SUB
    for v in range(nvar):
        coeff_ref[v, :, :deep] = spread(vertical_ref[v], 0)
        if v:
            coeff_ref[v, :, deep:] = spread(balance_ref[v - 1], 1)
    for first in range(0, size, WIDE):
        lanes = slice(first, first + WIDE)
        stream = None
        for v in range(nvar):
            block = blocks_ref[v, :, :, lanes].reshape(deep, WIDE)
            if v == 0:
                level = jnp.dot(coeff_ref[v, :, :deep], block, preferred_element_type=jnp.float32)
                level = stream = level.astype(jnp.bfloat16)
            else:
                level = jnp.dot(
                    coeff_ref[v],
                    jnp.concatenate([block, stream], axis=0),
                    preferred_element_type=jnp.float32,
                ).astype(jnp.bfloat16)
            shape = (out_ref.shape[1], out_ref.shape[2], SUB, WIDE)
            out_ref[v, :, :, :, lanes] = level.reshape(shape)


def mix_levels(blocks, vertical, balance, nmode):
    nvar, modes, _, size = blocks.shape
    tall = vertical.shape[2] * SUB
    each = tall // SUB // nmode
    return pl.pallas_call(
        level_kernel,
        out_shape=jax.ShapeDtypeStruct((nvar, nmode, each, SUB, size), jnp.bfloat16),
        scratch_shapes=[pltpu.VMEM((nvar, tall, modes * SUB + tall), jnp.bfloat16)],
        cost_estimate=cost(
            2 * tall * size * (nvar * modes * SUB + (nvar - 1) * tall), 8 * MB
        ),
        compiler_params=vmem(32),
        name="levels",
    )(blocks, vertical, balance)


def place_kernel(back_ref, out_any, sems):
    tiles, levs = back_ref.shape[:2]
    some = tiles // sems.shape[1]
    copies = []
    for at in range(levs):
        for i in range(sems.shape[1]):
            rows = pl.ds(i * some, some)
            copies.append(
                pltpu.make_async_copy(back_ref.at[rows, at], out_any.at[at, rows], sems.at[at, i])
            )
    for copy in copies:
        copy.start()
    for copy in copies:
        copy.wait()


def place(back):
    tiles, levs, sub, size = back.shape
    return pl.pallas_call(
        place_kernel,
        out_shape=jax.ShapeDtypeStruct((levs, tiles, sub, size), jnp.bfloat16),
        in_specs=[pl.BlockSpec(memory_space=pltpu.VMEM)],
        out_specs=pl.BlockSpec(memory_space=pl.ANY),
        scratch_shapes=[pltpu.SemaphoreType.DMA((levs, 8))],
        cost_estimate=cost(2**29, 8 * MB),
        compiler_params=vmem(16),
        name="place",
    )(back)


def per_device(control, filters, weights, vertical, balance):
    size = control.shape[-1]
    nmode, nvar = lax.axis_size("mode"), lax.axis_size("var")
    count = nmode * nvar
    each = vertical.shape[1] // nmode
    axes = ("var", "mode")
    filtered = smooth(control[0, 0, 0], filters, weights[0])
    blocks = lax.all_to_all(filtered.reshape(count, SUB, size), axes, 0, 0, tiled=True)
    result = mix_levels(blocks.reshape(nvar, nmode, SUB, size), jnp.swapaxes(vertical, 1, 2), balance, nmode)
    back = lax.all_to_all(result.reshape(count, each, SUB, size), axes, 0, 0, tiled=True)
    return place(back).reshape(1, 1, each, size, size)


def solution(mesh):
    in_specs = (P(None, "var", "mode", None, None), P(), P("var", None, None, None), P(), P())
    out_specs = P(None, "var", "mode", None, None)
    return jax.shard_map(
        per_device, mesh=mesh, in_specs=in_specs, out_specs=out_specs, check_vma=False
    )
```

```python
import jax
import jax.numpy as jnp
from jax import lax
from jax.experimental import pallas as pl
from jax.experimental.pallas import tpu as pltpu
from jax.sharding import PartitionSpec as P

SUB = 8
WIDE = 256
MB = 2**20


def vmem(mib):
    return pltpu.CompilerParams(vmem_limit_bytes=mib * MB)


def cost(flops, nbytes):
    return pl.CostEstimate(flops=int(flops), bytes_accessed=int(nbytes), transcendentals=0)


def spread(small, contract):
    cols = small.shape[contract]
    rows = small.shape[1 - contract]
    wide = cols * SUB
    lane = lax.broadcasted_iota(jnp.int32, (cols, wide), 1)
    source = lax.broadcasted_iota(jnp.int32, (cols, wide), 0)
    repeat = jnp.where(lane // SUB == source, 1.0, 0.0).astype(jnp.bfloat16)
    each = lax.dot_general(
        small, repeat, (((contract,), (0,)), ((), ())), preferred_element_type=jnp.float32
    )
    sub = lax.broadcasted_iota(jnp.int32, (rows, SUB, wide), 1)
    at = lax.broadcasted_iota(jnp.int32, (rows, SUB, wide), 2)
    tall = jnp.broadcast_to(each[:, None, :], (rows, SUB, wide))
    return jnp.where(at % SUB == sub, tall, 0.0).reshape(rows * SUB, wide).astype(jnp.bfloat16)


def smooth_kernel(
    plane_any, filters_any, weights_any,
    out_ref,
    plane_ref, filters_ref, weights_ref, half_ref, total_ref,
    sems,
):
    count = filters_ref.shape[0]
    plane = pltpu.make_async_copy(plane_any, plane_ref, sems.at[2 * count])
    middle = filters_ref.shape[1] // 2
    first, second = pl.ds(0, middle), pl.ds(middle, middle)
    filters = [
        pltpu.make_async_copy(filters_any.at[k], filters_ref.at[k], sems.at[2 * k])
        for k in range(1, count)
    ]
    halves = [
        pltpu.make_async_copy(filters_any.at[0, at], filters_ref.at[0, at], sems.at[where])
        for at, where in ((first, 0), (second, 2 * count + 1))
    ]
    weights = [
        pltpu.make_async_copy(weights_any.at[k], weights_ref.at[k], sems.at[2 * k + 1])
        for k in range(count)
    ]
    plane.start()
    for copy in halves + weights[:1]:
        copy.start()
    for k in range(1, count):
        filters[k - 1].start()
        weights[k].start()

    plane.wait()
    for k in range(count):
        if k:
            filters[k - 1].wait()
            half_ref[...] = jnp.dot(
                filters_ref[k], plane_ref[...], preferred_element_type=jnp.float32
            ).astype(jnp.bfloat16)
        else:
            for copy, at in zip(halves, (first, second)):
                copy.wait()
                half_ref[at, :] = jnp.dot(
                    filters_ref[0, at, :], plane_ref[...], preferred_element_type=jnp.float32
                ).astype(jnp.bfloat16)
        weights[k].wait()
        full = lax.dot_general(
            half_ref[...], filters_ref[k], (((1,), (1,)), ((), ())),
            preferred_element_type=jnp.float32,
        )
        term = weights_ref[k].astype(jnp.float32) * full
        if k == 0:
            total_ref[...] = term
        elif k < count - 1:
            total_ref[...] += term
        else:
            out_ref[...] = (total_ref[...] + term).astype(jnp.bfloat16)


def smooth(plane, filters, weights):
    count, size, _ = filters.shape
    return pl.pallas_call(
        smooth_kernel,
        out_shape=jax.ShapeDtypeStruct((size, size), jnp.bfloat16),
        in_specs=[pl.BlockSpec(memory_space=pl.ANY)] * 3,
        scratch_shapes=[
            pltpu.VMEM(plane.shape, jnp.bfloat16),
            pltpu.VMEM(filters.shape, jnp.bfloat16),
            pltpu.VMEM(weights.shape, jnp.bfloat16),
            pltpu.VMEM((size, size), jnp.bfloat16),
            pltpu.VMEM((size, size), jnp.float32),
            pltpu.SemaphoreType.DMA((2 * count + 2,)),
        ],
        cost_estimate=cost(4 * count * size**3, 18 * MB),
        compiler_params=pltpu.CompilerParams(vmem_limit_bytes=52428800),
        name="smooth",
    )(plane, filters, weights)


def level_kernel(blocks_ref, vertical_ref, balance_ref, out_ref, coeff_ref):
    nvar, modes, _, size = blocks_ref.shape
    deep = modes * SUB
    for v in range(nvar):
        coeff_ref[v, :, :deep] = spread(vertical_ref[v], 0)
        if v:
            coeff_ref[v, :, deep:] = spread(balance_ref[v - 1], 1)
    for first in range(0, size, WIDE):
        lanes = slice(first, first + WIDE)
        stream = None
        for v in range(nvar):
            block = blocks_ref[v, :, :, lanes].reshape(deep, WIDE)
            if v == 0:
                level = jnp.dot(coeff_ref[v, :, :deep], block, preferred_element_type=jnp.float32)
                level = stream = level.astype(jnp.bfloat16)
            else:
                level = jnp.dot(
                    coeff_ref[v],
                    jnp.concatenate([block, stream], axis=0),
                    preferred_element_type=jnp.float32,
                ).astype(jnp.bfloat16)
            shape = (out_ref.shape[1], out_ref.shape[2], SUB, WIDE)
            out_ref[v, :, :, :, lanes] = level.reshape(shape)


def mix_levels(blocks, vertical, balance, nmode):
    nvar, modes, _, size = blocks.shape
    tall = vertical.shape[2] * SUB
    each = tall // SUB // nmode
    return pl.pallas_call(
        level_kernel,
        out_shape=jax.ShapeDtypeStruct((nvar, nmode, each, SUB, size), jnp.bfloat16),
        scratch_shapes=[pltpu.VMEM((nvar, tall, modes * SUB + tall), jnp.bfloat16)],
        cost_estimate=cost(
            2 * tall * size * (nvar * modes * SUB + (nvar - 1) * tall), 8 * MB
        ),
        compiler_params=vmem(32),
        name="levels",
    )(blocks, vertical, balance)


def place_kernel(back_ref, out_any, sems):
    tiles, levs = back_ref.shape[:2]
    some = tiles // sems.shape[1]
    copies = []
    for at in range(levs):
        for i in range(sems.shape[1]):
            rows = pl.ds(i * some, some)
            copies.append(
                pltpu.make_async_copy(back_ref.at[rows, at], out_any.at[at, rows], sems.at[at, i])
            )
    for copy in copies:
        copy.start()
    for copy in copies:
        copy.wait()


def place(back):
    tiles, levs, sub, size = back.shape
    return pl.pallas_call(
        place_kernel,
        out_shape=jax.ShapeDtypeStruct((levs, tiles, sub, size), jnp.bfloat16),
        in_specs=[pl.BlockSpec(memory_space=pltpu.VMEM)],
        out_specs=pl.BlockSpec(memory_space=pl.ANY),
        scratch_shapes=[pltpu.SemaphoreType.DMA((levs, 8))],
        cost_estimate=cost(2**29, 8 * MB),
        compiler_params=vmem(16),
        name="place",
    )(back)


def per_device(control, filters, weights, vertical, balance):
    size = control.shape[-1]
    nmode, nvar = lax.axis_size("mode"), lax.axis_size("var")
    count = nmode * nvar
    each = vertical.shape[1] // nmode
    axes = ("var", "mode")
    filtered = smooth(control[0, 0, 0], filters, weights[0])
    blocks = lax.all_to_all(filtered.reshape(count, SUB, size), axes, 0, 0, tiled=True)
    result = mix_levels(blocks.reshape(nvar, nmode, SUB, size), jnp.swapaxes(vertical, 1, 2), balance, nmode)
    back = lax.all_to_all(result.reshape(count, each, SUB, size), axes, 0, 0, tiled=True)
    return place(back).reshape(1, 1, each, size, size)


def solution(mesh):
    in_specs = (P(None, "var", "mode", None, None), P(), P("var", None, None, None), P(), P())
    out_specs = P(None, "var", "mode", None, None)
    return jax.shard_map(
        per_device, mesh=mesh, in_specs=in_specs, out_specs=out_specs, check_vma=False
    )
```
